32 devices in a mesh: member: 2 (over x), dp: 16 (over z, y, core).
Axes of the slice: x: 2, y: 2, z: 4, core: 2. Of those that a mesh axis runs over, the one named last changes fastest.
Arguments:
- residual: bfloat16 [512, 3072], P(('member', 'dp')), parts along dimension 0, may hold values from -6 to 6
- upstream: bfloat16 [512, 3072], P(('member', 'dp')), parts along dimension 0, may hold values from -6 to 6
- gate_weight: bfloat16 [6144, 10240], P('member', 'dp'), parts along dimension 0, may hold values from -0.109375 to 0.109375
- up_weight: bfloat16 [6144, 10240], P('member', 'dp'), parts along dimension 0, may hold values from -0.109375 to 0.109375
- down_weight: bfloat16 [20480, 3072], P(('member', 'dp')), parts along dimension 0, may hold values from -0.0625 to 0.0625
- gain: float32 [6144], P('member'), parts along dimension 0, may hold values from 0.25 to 1.75
Outputs:
- grad_residual: bfloat16 [512, 3072], P(('member', 'dp')), parts along dimension 0
- grad_gate: bfloat16 [6144, 10240], P('member', 'dp'), parts along dimension 0
- grad_up: bfloat16 [6144, 10240], P('member', 'dp'), parts along dimension 0
- grad_down: bfloat16 [20480, 3072], P(('member', 'dp')), parts along dimension 0
- grad_gain: float32 [6144], P('member'), parts along dimension 0
The draws below stay inside these ranges and needn't reach their ends.
There are 2 independent parts, one for each index of `member`. The reference program is written for one: setup_inputs(seed, part) draws one part's arguments, and reference() takes and returns one part's arrays. A program takes and returns all parts, laid end to end along the dimension named above; each array names one. Nothing has to cross between parts.
All inputs are finite; a program needn't handle non-finite values.
Results may differ from the reference program's by a relative error of at most 0.0068.
Values may be sent and summed in bfloat16 or wider, within the bound.
A program may use at most 128 MiB of HBM per device.

```python
import jax
import jax.numpy as jnp
from jax import lax

D = 3072
FF = 10240
TOKENS = 256


def block_scale(stream_key, dims, pieces, smallest, high):
    level, own = 1.0, jax.random.fold_in(stream_key, 6)
    for dim, blocks in pieces:
        steps = jnp.exp(jax.random.uniform(jax.random.fold_in(own, dim), (blocks,), jnp.float32, smallest / len(pieces), high / len(pieces)))
        level = level * jnp.repeat(steps, dims[dim] // blocks).reshape([-1 if axis == dim else 1 for axis in range(len(dims))])
    return level


def normal_values(key, shape, scale, most, split=(), held_as=jnp.bfloat16):
    entries = jax.random.normal(key, shape, jnp.float32) * scale
    if len(split) > 0:
        entries = block_scale(key, shape, split, -0.22, 0.18) * entries
    return jnp.clip(entries, min=-most, max=most).astype(held_as)


def setup_inputs(seed: int = 0, part: int = 0) -> dict:
    key_of = jax.random.split(jax.random.key(seed), 7)
    own_keys = jax.random.split(jax.random.fold_in(key_of[6], part), 7)
    return {
        "residual": normal_values(own_keys[0], (TOKENS, D), 1.0, 6.0, ((0, 16),)),
        "upstream": normal_values(own_keys[1], (TOKENS, D), 1.0, 6.0, ((0, 16),)),
        "gate_weight": normal_values(own_keys[2], (D, FF), D ** -0.5, 0.109375, ((1, 16),)),
        "up_weight": normal_values(own_keys[3], (D, FF), D ** -0.5, 0.109375, ((1, 16),)),
        "down_weight": normal_values(own_keys[4], (FF, D), FF ** -0.5, 0.0625, ((0, 16),)),
        "gain": jnp.clip(1.0 + 0.15 * jax.random.normal(own_keys[5], (D,), jnp.float32), 0.25, 1.75),
    }


norm_floor = 0.5
gelu_coeff = 0.7978845608
cubic_term = 0.044715

def gelu_parts(gate_out):
    inner = jnp.tanh(gelu_coeff * (gate_out + cubic_term * gate_out * gate_out * gate_out))
    activated = 0.5 * gate_out * (1.0 + inner)
    gelu_slope = 0.5 * (1.0 + inner) + 0.5 * gate_out * (1.0 - inner * inner) * gelu_coeff * (1.0 + 3.0 * cubic_term * gate_out * gate_out)
    return (activated, gelu_slope)

def contract_last(left, right):
    return lax.dot_general(left, right, (((1,), (1,)), ((), ())), preferred_element_type=jnp.float32)

def contract_first(left, right):
    return lax.dot_general(left, right, (((0,), (0,)), ((), ())), preferred_element_type=jnp.float32)

def reference(residual, upstream, gate_weight, up_weight, down_weight, gain):
    widened = residual.astype(jnp.float32)
    norm_scale = lax.rsqrt(lax.optimization_barrier(jnp.mean(widened * widened, axis=1, keepdims=True)) + norm_floor)
    unit_rows = widened * norm_scale
    normed = (unit_rows * gain).astype(jnp.bfloat16)
    gate_out = jnp.dot(normed, gate_weight, preferred_element_type=jnp.float32)
    up_out = jnp.dot(normed, up_weight, preferred_element_type=jnp.float32)
    activated, gelu_slope = gelu_parts(gate_out)
    hidden = (activated * up_out).astype(jnp.bfloat16)
    hidden_grad = contract_last(upstream, down_weight)
    grad_down = contract_first(hidden, upstream).astype(jnp.bfloat16)
    gate_grad = (hidden_grad * up_out * gelu_slope).astype(jnp.bfloat16)
    up_grad = (hidden_grad * activated).astype(jnp.bfloat16)
    grad_gate = contract_first(normed, gate_grad).astype(jnp.bfloat16)
    grad_up = contract_first(normed, up_grad).astype(jnp.bfloat16)
    normed_grad = contract_last(gate_grad, gate_weight) + contract_last(up_grad, up_weight)
    unit_grad = normed_grad * gain
    inner_mean = lax.optimization_barrier(jnp.mean(unit_grad * unit_rows, axis=1, keepdims=True))
    grad_residual = (upstream.astype(jnp.float32) + norm_scale * (unit_grad - unit_rows * inner_mean)).astype(jnp.bfloat16)
    grad_gain = lax.optimization_barrier(jnp.sum(normed_grad * unit_rows, axis=0))
    return (grad_residual, grad_gate, grad_up, grad_down, grad_gain)
```

```python
import functools

import jax
import jax.numpy as jnp
from jax import lax
from jax.experimental import pallas as pl
from jax.experimental.pallas import tpu as pltpu
from jax.sharding import PartitionSpec as P

norm_floor = 0.5
gelu_coeff = 0.7978845608
cubic_term = 0.044715
MESH = pl.DeviceIdType.MESH
bf16, f32 = jnp.bfloat16, jnp.float32


def gelu_parts(gate_out):
    inner = jnp.tanh(gelu_coeff * (gate_out + cubic_term * gate_out * gate_out * gate_out))
    activated = 0.5 * gate_out * (1.0 + inner)
    gelu_slope = 0.5 * (1.0 + inner) + 0.5 * gate_out * (1.0 - inner * inner) * gelu_coeff * (
        1.0 + 3.0 * cubic_term * gate_out * gate_out
    )
    return (activated, gelu_slope)


def contract_last(left, right):
    return lax.dot_general(left, right, (((1,), (1,)), ((), ())), preferred_element_type=f32)


def contract_first(left, right):
    return lax.dot_general(left, right, (((0,), (0,)), ((), ())), preferred_element_type=f32)


def slot(side, distance, half_ring):
    if distance == half_ring:
        return 2 * half_ring - 1
    return 0 if distance == 0 else 2 * distance - 1 + side


def exchange_kernel(
    chips,
    res_hbm, ups_hbm, gate_hbm, up_hbm, down_hbm, gain_ref,
    grad_res_ref, gain_out_ref, normed_hbm, upstream_hbm, hidden_hbm, gate_grad_hbm, up_grad_hbm,
    gate_w, up_w, down_w, res, ups, normed, scale, hidden, gate_grad, up_grad,
    part, peer_send, peer_recv, ring_send, ring_recv,
    gain_part, gain_peer, gain_sum, gain_all, gain_full,
    local_sem, out_sem, own_sem, ring_ss, ring_rs, peer_ss, peer_rs,
    swap_ss, swap_rs, sum_ss, sum_rs, gain_ss, gain_rs,
):
    half_ring = chips // 2
    rows = res_hbm.shape[0]
    width = res.shape[1]
    half_width = width // 2
    tokens = res.shape[0]
    me = lax.axis_index("dp")
    chip, core = me // 2, me % 2
    position = chip // 2 + (chip % 2) * (chips - 1 - 2 * (chip // 2))

    def device_at(place, which):
        place = (place + chips) % chips
        far = place // half_ring
        return 2 * ((1 - far) * (2 * place) + far * (2 * (chips - 1 - place) + 1)) + which

    partner = {"dp": 2 * chip + (1 - core)}
    onward = ({"dp": device_at(position + 1, core)}, {"dp": device_at(position - 1, core)})

    def block(ref, k, who):
        return ref.at[pl.ds((2 * k + who) * rows, rows)]

    sources, arrays = (res_hbm, ups_hbm), (res, ups)
    own = [pltpu.make_async_copy(sources[a], block(arrays[a], 0, 0), own_sem.at[a]) for a in (0, 1)]
    for copy in own:
        copy.start()
    weights = [
        pltpu.make_async_copy(src, dst, local_sem.at[i])
        for i, (src, dst) in enumerate(((gate_hbm, gate_w), (up_hbm, up_w), (down_hbm, down_w)))
    ]
    for copy in weights:
        copy.start()

    barrier = pltpu.get_barrier_semaphore()
    pl.semaphore_signal(barrier, inc=1, device_id=partner, device_id_type=MESH)
    for step in range(1, chips):
        pl.semaphore_signal(
            barrier, inc=1, device_id={"dp": device_at(position + step, core)}, device_id_type=MESH
        )
    pl.semaphore_wait(barrier, chips)
    for copy in own:
        copy.wait()

    def remote(src, dst, send, recv, target):
        return pltpu.make_async_remote_copy(
            src_ref=src, dst_ref=dst, send_sem=send, recv_sem=recv,
            device_id=target, device_id_type=MESH,
        )

    def reach(direction, a):
        return half_ring if direction == a else half_ring - 1

    def hop(direction, a, distance):
        return remote(
            block(arrays[a], slot(direction, distance, half_ring), 0),
            block(arrays[a], slot(direction, distance + 1, half_ring), 0),
            ring_ss.at[direction, a, distance],
            ring_rs.at[direction, a, distance],
            onward[direction],
        )

    def share(a, k):
        return remote(
            block(arrays[a], k, 0), block(arrays[a], k, 1),
            peer_ss.at[a, k], peer_rs.at[a, k], partner,
        )

    streams = [(0, 0), (1, 0), (0, 1), (1, 1)]
    for direction, a in streams:
        hop(direction, a, 0).start()
    for a in (0, 1):
        share(a, 0).start()

    def arrive(distance):
        for direction, a in streams:
            if distance > reach(direction, a):
                continue
            hop(direction, a, distance - 1).wait_recv()
            if distance < reach(direction, a):
                hop(direction, a, distance).start()
            share(a, slot(direction, distance, half_ring)).start()

    batch = chips // 2
    span = batch * 2 * rows

    def normalise(b):
        for k in range(b * batch, (b + 1) * batch):
            share(0, k).wait_recv()
            at = pl.ds(2 * k * rows, 2 * rows)
            wide = res[at, :].astype(f32)
            own_scale = lax.rsqrt(jnp.mean(wide * wide, axis=1, keepdims=True) + norm_floor)
            scale[at, :] = own_scale
            normed[at, :] = (wide * own_scale * gain_ref[...]).astype(bf16)

    def forward(b):
        at = pl.ds(b * span, span)
        rows_in = normed[at, :]
        gate_out = jnp.dot(rows_in, gate_w[...], preferred_element_type=f32)
        up_out = jnp.dot(rows_in, up_w[...], preferred_element_type=f32)
        for k in range(b * batch, (b + 1) * batch):
            share(1, k).wait_recv()
        hidden_grad = contract_last(ups[at, :], down_w[...])
        activated, gelu_slope = gelu_parts(gate_out)
        hidden[at, :] = (activated * up_out).astype(bf16)
        gate_grad[at, :] = (hidden_grad * up_out * gelu_slope).astype(bf16)
        up_grad[at, :] = (hidden_grad * activated).astype(bf16)

    def backward(b):
        at = pl.ds(b * span, span)
        part[at, :] = contract_last(gate_grad[at, :], gate_w[...]) + contract_last(
            up_grad[at, :], up_w[...]
        )
        for k in range(b * batch, (b + 1) * batch):
            peer_send[pl.ds(k * rows, rows), :] = part[pl.ds((2 * k + 1) * rows, rows), :].astype(bf16)
        swap(b).start()

    def swap(b):
        at = pl.ds(b * batch * rows, batch * rows)
        return remote(peer_send.at[at], peer_recv.at[at], swap_ss.at[b], swap_rs.at[b], partner)

    def gain_term(b):
        total = jnp.zeros((1, width), f32)
        for k in range(b * batch, (b + 1) * batch):
            at = pl.ds(2 * k * rows, 2 * rows)
            unit_rows = res[at, :].astype(f32) * scale[at, :]
            total = total + jnp.sum(part[at, :] * unit_rows, axis=0, keepdims=True)
        return total

    early = (half_ring + 1) // 2
    for distance in range(1, early + 1):
        arrive(distance)
    for copy in weights:
        copy.wait()
    normalise(0)
    forward(0)
    for distance in range(early + 1, half_ring):
        arrive(distance)
    backward(0)
    gain_total = gain_term(0)
    arrive(half_ring)
    normalise(1)
    forward(1)
    backward(1)

    outs = [
        pltpu.make_async_copy(src, dst, out_sem.at[i])
        for i, (src, dst) in enumerate(
            (
                (normed, normed_hbm), (ups, upstream_hbm), (hidden, hidden_hbm),
                (gate_grad, gate_grad_hbm), (up_grad, up_grad_hbm),
            )
        )
    ]
    for copy in outs:
        copy.start()

    def pass_on(direction, h, distance):
        return remote(
            ring_send.at[direction, h, distance - 1],
            ring_recv.at[direction, h, distance - 1],
            sum_ss.at[direction, h, distance - 1],
            sum_rs.at[direction, h, distance - 1],
            onward[direction],
        )

    def columns(h):
        return pl.ds(h * half_width, half_width)

    def held(k, h):
        return part[pl.ds(2 * k * rows, rows), columns(h)] + peer_recv[
            pl.ds(k * rows, rows), columns(h)
        ].astype(f32)

    ring_order = [(0, 0), (1, 1), (1, 0), (0, 1)]

    def sum_step(distance):
        for direction, h in ring_order:
            if distance > reach(direction, h):
                continue
            value = held(slot(1 - direction, distance, half_ring), h)
            if distance < reach(direction, h):
                pass_on(direction, h, distance + 1).wait_recv()
                value = value + ring_recv[direction, h, distance].astype(f32)
            ring_send[direction, h, distance - 1] = value.astype(bf16)
            pass_on(direction, h, distance).start()

    swap(1).wait_recv()
    sum_step(half_ring)

    gain_total = gain_total + gain_term(1)
    gain_part[0] = gain_total[:, :half_width]
    gain_part[1] = gain_total[:, half_width:]
    gain_swap = remote(gain_part.at[1 - core], gain_peer, gain_ss.at[0], gain_rs.at[0], partner)
    gain_swap.start()
    swap(0).wait_recv()

    sum_step(half_ring - 1)
    gain_swap.wait_recv()
    gain_sum[...] = gain_part[core] + gain_peer[...]
    spread = [
        remote(
            gain_sum, gain_all.at[step - 1], gain_ss.at[step], gain_rs.at[step],
            {"dp": device_at(position + step, core)},
        )
        for step in range(1, chips)
    ]
    for copy in spread:
        copy.start()
    for distance in range(half_ring - 2, 0, -1):
        sum_step(distance)

    gain_value = gain_sum[...]
    for step in range(1, chips):
        spread[step - 1].wait_recv()
        gain_value = gain_value + gain_all[step - 1]
    gain_full[core] = gain_value
    gain_back = remote(
        gain_full.at[core], gain_full.at[core], gain_ss.at[chips], gain_rs.at[chips], partner
    )
    gain_back.start()

    for direction, h in ring_order:
        pass_on(direction, h, 1).wait_recv()
    normed_grad = jnp.concatenate(
        [
            held(0, h) + ring_recv[0, h, 0].astype(f32) + ring_recv[1, h, 0].astype(f32)
            for h in (0, 1)
        ],
        axis=1,
    )
    first = pl.ds(0, rows)
    norm_scale = scale[first, :]
    unit_rows = res[first, :].astype(f32) * norm_scale
    unit_grad = normed_grad * gain_ref[...]
    inner_mean = jnp.mean(unit_grad * unit_rows, axis=1, keepdims=True)
    grad_res_ref[...] = (
        ups[first, :].astype(f32) + norm_scale * (unit_grad - unit_rows * inner_mean)
    ).astype(bf16)

    gain_back.wait_recv()
    gain_out_ref[...] = gain_full[...]

    for direction, a in streams:
        for distance in range(reach(direction, a)):
            hop(direction, a, distance).wait_send()
            pass_on(direction, a, distance + 1).wait_send()
    for a in (0, 1):
        for k in range(chips):
            share(a, k).wait_send()
        swap(a).wait_send()
    gain_swap.wait_send()
    gain_back.wait_send()
    for copy in spread:
        copy.wait_send()
    for copy in outs:
        copy.wait()


def per_device(chips, residual, upstream, gate_weight, up_weight, down_weight, gain):
    rows, width = residual.shape
    units = gate_weight.shape[1]
    tokens = rows * 2 * chips
    half_ring = chips // 2
    shape = jax.ShapeDtypeStruct
    anywhere = pl.BlockSpec(memory_space=pl.ANY)
    in_vmem = pl.BlockSpec(memory_space=pltpu.VMEM)
    dma = pltpu.SemaphoreType.DMA
    grad_residual, grad_gain, normed, upstream_all, hidden, gate_grad, up_grad = pl.pallas_call(
        functools.partial(exchange_kernel, chips),
        out_shape=(
            shape((rows, width), bf16),
            shape((2, 1, width // 2), f32),
            shape((tokens, width), bf16),
            shape((tokens, width), bf16),
            shape((tokens, units), bf16),
            shape((tokens, units), bf16),
            shape((tokens, units), bf16),
        ),
        in_specs=[anywhere] * 5 + [in_vmem],
        out_specs=(in_vmem, in_vmem) + (anywhere,) * 5,
        scratch_shapes=[
            pltpu.VMEM((width, units), bf16),
            pltpu.VMEM((width, units), bf16),
            pltpu.VMEM((units, width), bf16),
            pltpu.VMEM((tokens, width), bf16),
            pltpu.VMEM((tokens, width), bf16),
            pltpu.VMEM((tokens, width), bf16),
            pltpu.VMEM((tokens, 1), f32),
            pltpu.VMEM((tokens, units), bf16),
            pltpu.VMEM((tokens, units), bf16),
            pltpu.VMEM((tokens, units), bf16),
            pltpu.VMEM((tokens, width), f32),
            pltpu.VMEM((tokens // 2, width), bf16),
            pltpu.VMEM((tokens // 2, width), bf16),
            pltpu.VMEM((2, 2, half_ring, rows, width // 2), bf16),
            pltpu.VMEM((2, 2, half_ring, rows, width // 2), bf16),
            pltpu.VMEM((2, 1, width // 2), f32),
            pltpu.VMEM((1, width // 2), f32),
            pltpu.VMEM((1, width // 2), f32),
            pltpu.VMEM((chips - 1, 1, width // 2), f32),
            pltpu.VMEM((2, 1, width // 2), f32),
            dma((3,)),
            dma((5,)),
            dma((2,)),
            dma((2, 2, half_ring)),
            dma((2, 2, half_ring)),
            dma((2, chips)),
            dma((2, chips)),
            dma((2,)),
            dma((2,)),
            dma((2, 2, half_ring)),
            dma((2, 2, half_ring)),
            dma((chips + 1,)),
            dma((chips + 1,)),
        ],
        compiler_params=pltpu.CompilerParams(
            collective_id=0, has_side_effects=True, vmem_limit_bytes=60 * 1024 * 1024
        ),
    )(residual, upstream, gate_weight, up_weight, down_weight, gain.reshape(1, width))
    grad_gate = contract_first(normed, gate_grad).astype(bf16)
    grad_up = contract_first(normed, up_grad).astype(bf16)
    grad_down = contract_first(hidden, upstream_all).astype(bf16)
    return (grad_residual, grad_gate, grad_up, grad_down, grad_gain.reshape(width))


def solution(mesh):
    placed = (
        P(("member", "dp"), None),
        P(("member", "dp"), None),
        P("member", "dp"),
        P("member", "dp"),
        P(("member", "dp"), None),
        P("member"),
    )
    return jax.shard_map(
        functools.partial(per_device, mesh.shape["dp"] // 2),
        mesh=mesh,
        in_specs=placed,
        out_specs=(
            P(("member", "dp"), None),
            P("member", "dp"),
            P("member", "dp"),
            P(("member", "dp"), None),
            P("member"),
        ),
        check_vma=False,
    )
```

```python
import functools

import jax
import jax.numpy as jnp
from jax import lax
from jax.experimental import pallas as pl
from jax.experimental.pallas import tpu as pltpu
from jax.sharding import PartitionSpec as P

norm_floor = 0.5
gelu_coeff = 0.7978845608
cubic_term = 0.044715
MESH = pl.DeviceIdType.MESH
bf16, f32 = jnp.bfloat16, jnp.float32


def gelu_parts(gate_out):
    inner = jnp.tanh(gelu_coeff * (gate_out + cubic_term * gate_out * gate_out * gate_out))
    activated = 0.5 * gate_out * (1.0 + inner)
    gelu_slope = 0.5 * (1.0 + inner) + 0.5 * gate_out * (1.0 - inner * inner) * gelu_coeff * (
        1.0 + 3.0 * cubic_term * gate_out * gate_out
    )
    return (activated, gelu_slope)


def contract_last(left, right):
    return lax.dot_general(left, right, (((1,), (1,)), ((), ())), preferred_element_type=f32)


def contract_first(left, right):
    return lax.dot_general(left, right, (((0,), (0,)), ((), ())), preferred_element_type=f32)


def slot(side, distance, half_ring):
    if distance == half_ring:
        return 2 * half_ring - 1
    return 0 if distance == 0 else 2 * distance - 1 + side


def exchange_kernel(
    chips,
    res_hbm, ups_hbm, gate_hbm, up_hbm, down_hbm, gain_ref,
    grad_res_ref, gain_out_ref, normed_hbm, upstream_hbm, hidden_hbm, gate_grad_hbm, up_grad_hbm,
    gate_w, up_w, down_w, res, ups, normed, normed_t, scale, hidden, gate_grad, up_grad,
    part, peer_send, peer_recv, ring_send, ring_recv,
    gain_part, gain_peer, gain_sum, gain_all, gain_full,
    local_sem, out_sem, own_sem, ring_ss, ring_rs, peer_ss, peer_rs,
    swap_ss, swap_rs, sum_ss, sum_rs, gain_ss, gain_rs,
):
    half_ring = chips // 2
    rows = res_hbm.shape[0]
    width = res.shape[1]
    half_width = width // 2
    tokens = res.shape[0]
    me = lax.axis_index("dp")
    chip, core = me // 2, me % 2
    position = chip // 2 + (chip % 2) * (chips - 1 - 2 * (chip // 2))

    def device_at(place, which):
        place = (place + chips) % chips
        far = place // half_ring
        return 2 * ((1 - far) * (2 * place) + far * (2 * (chips - 1 - place) + 1)) + which

    partner = {"dp": 2 * chip + (1 - core)}
    onward = ({"dp": device_at(position + 1, core)}, {"dp": device_at(position - 1, core)})

    def block(ref, k, who):
        return ref.at[pl.ds((2 * k + who) * rows, rows)]

    sources, arrays = (res_hbm, ups_hbm), (res, ups)
    own = [pltpu.make_async_copy(sources[a], block(arrays[a], 0, 0), own_sem.at[a]) for a in (0, 1)]
    for copy in own:
        copy.start()
    weights = [
        pltpu.make_async_copy(src, dst, local_sem.at[i])
        for i, (src, dst) in enumerate(((gate_hbm, gate_w), (up_hbm, up_w), (down_hbm, down_w)))
    ]
    for copy in weights:
        copy.start()

    barrier = pltpu.get_barrier_semaphore()
    pl.semaphore_signal(barrier, inc=1, device_id=partner, device_id_type=MESH)
    for step in range(1, chips):
        pl.semaphore_signal(
            barrier, inc=1, device_id={"dp": device_at(position + step, core)}, device_id_type=MESH
        )
    pl.semaphore_wait(barrier, chips)
    for copy in own:
        copy.wait()

    def remote(src, dst, send, recv, target):
        return pltpu.make_async_remote_copy(
            src_ref=src, dst_ref=dst, send_sem=send, recv_sem=recv,
            device_id=target, device_id_type=MESH,
        )

    def reach(direction, a):
        return half_ring if direction == a else half_ring - 1

    def hop(direction, a, distance):
        return remote(
            block(arrays[a], slot(direction, distance, half_ring), 0),
            block(arrays[a], slot(direction, distance + 1, half_ring), 0),
            ring_ss.at[direction, a, distance],
            ring_rs.at[direction, a, distance],
            onward[direction],
        )

    def share(a, k):
        return remote(
            block(arrays[a], k, 0), block(arrays[a], k, 1),
            peer_ss.at[a, k], peer_rs.at[a, k], partner,
        )

    streams = [(0, 0), (1, 0), (0, 1), (1, 1)]
    for direction, a in streams:
        hop(direction, a, 0).start()
    for a in (0, 1):
        share(a, 0).start()

    def arrive(distance):
        for direction, a in streams:
            if distance > reach(direction, a):
                continue
            hop(direction, a, distance - 1).wait_recv()
            if distance < reach(direction, a):
                hop(direction, a, distance).start()
            share(a, slot(direction, distance, half_ring)).start()

    batch = chips // 2
    span = batch * 2 * rows

    def normalise(b):
        for k in range(b * batch, (b + 1) * batch):
            share(0, k).wait_recv()
            at = pl.ds(2 * k * rows, 2 * rows)
            wide = res[at, :].astype(f32)
            own_scale = lax.rsqrt(jnp.mean(wide * wide, axis=1, keepdims=True) + norm_floor)
            scale[at, :] = own_scale
            normed[at, :] = (wide * own_scale * gain_ref[...]).astype(bf16)

    def forward(b):
        at = pl.ds(b * span, span)
        rows_in = normed[at, :]
        gate_out = jnp.dot(rows_in, gate_w[...], preferred_element_type=f32)
        up_out = jnp.dot(rows_in, up_w[...], preferred_element_type=f32)
        for k in range(b * batch, (b + 1) * batch):
            share(1, k).wait_recv()
        hidden_grad = contract_last(ups[at, :], down_w[...])
        activated, gelu_slope = gelu_parts(gate_out)
        hidden[:, at] = (activated * up_out).T.astype(bf16)
        gate_grad[at, :] = (hidden_grad * up_out * gelu_slope).astype(bf16)
        up_grad[at, :] = (hidden_grad * activated).astype(bf16)

    def backward(b):
        at = pl.ds(b * span, span)
        part[at, :] = contract_last(gate_grad[at, :], gate_w[...]) + contract_last(
            up_grad[at, :], up_w[...]
        )
        for k in range(b * batch, (b + 1) * batch):
            peer_send[pl.ds(k * rows, rows), :] = part[pl.ds((2 * k + 1) * rows, rows), :].astype(bf16)
        swap(b).start()

    def swap(b):
        at = pl.ds(b * batch * rows, batch * rows)
        return remote(peer_send.at[at], peer_recv.at[at], swap_ss.at[b], swap_rs.at[b], partner)

    def turn(b):
        at = pl.ds(b * span, span)
        normed_t[:, at] = normed[at, :].T

    def gain_term(b):
        total = jnp.zeros((1, width), f32)
        for k in range(b * batch, (b + 1) * batch):
            at = pl.ds(2 * k * rows, 2 * rows)
            unit_rows = res[at, :].astype(f32) * scale[at, :]
            total = total + jnp.sum(part[at, :] * unit_rows, axis=0, keepdims=True)
        return total

    early = (half_ring + 1) // 2
    for distance in range(1, early + 1):
        arrive(distance)
    for copy in weights:
        copy.wait()
    normalise(0)
    forward(0)
    for distance in range(early + 1, half_ring):
        arrive(distance)
    backward(0)
    gain_total = gain_term(0)
    turn(0)
    arrive(half_ring)
    normalise(1)
    forward(1)
    backward(1)

    def pass_on(direction, h, distance):
        return remote(
            ring_send.at[direction, h, distance - 1],
            ring_recv.at[direction, h, distance - 1],
            sum_ss.at[direction, h, distance - 1],
            sum_rs.at[direction, h, distance - 1],
            onward[direction],
        )

    def columns(h):
        return pl.ds(h * half_width, half_width)

    def held(k, h):
        return part[pl.ds(2 * k * rows, rows), columns(h)] + peer_recv[
            pl.ds(k * rows, rows), columns(h)
        ].astype(f32)

    ring_order = [(0, 0), (1, 1), (1, 0), (0, 1)]

    def sum_step(distance):
        for direction, h in ring_order:
            if distance > reach(direction, h):
                continue
            value = held(slot(1 - direction, distance, half_ring), h)
            if distance < reach(direction, h):
                pass_on(direction, h, distance + 1).wait_recv()
                value = value + ring_recv[direction, h, distance].astype(f32)
            ring_send[direction, h, distance - 1] = value.astype(bf16)
            pass_on(direction, h, distance).start()

    swap(1).wait_recv()
    sum_step(half_ring)

    gain_total = gain_total + gain_term(1)
    gain_part[0] = gain_total[:, :half_width]
    gain_part[1] = gain_total[:, half_width:]
    gain_swap = remote(gain_part.at[1 - core], gain_peer, gain_ss.at[0], gain_rs.at[0], partner)
    gain_swap.start()
    swap(0).wait_recv()

    sum_step(half_ring - 1)
    turn(1)
    outs = [
        pltpu.make_async_copy(src, dst, out_sem.at[i])
        for i, (src, dst) in enumerate(
            (
                (normed_t, normed_hbm), (ups, upstream_hbm), (hidden, hidden_hbm),
                (gate_grad, gate_grad_hbm), (up_grad, up_grad_hbm),
            )
        )
    ]
    for copy in outs:
        copy.start()

    gain_swap.wait_recv()
    gain_sum[...] = gain_part[core] + gain_peer[...]
    spread = [
        remote(
            gain_sum, gain_all.at[step - 1], gain_ss.at[step], gain_rs.at[step],
            {"dp": device_at(position + step, core)},
        )
        for step in range(1, chips)
    ]
    for copy in spread:
        copy.start()
    for distance in range(half_ring - 2, 0, -1):
        sum_step(distance)

    gain_value = gain_sum[...]
    for step in range(1, chips):
        spread[step - 1].wait_recv()
        gain_value = gain_value + gain_all[step - 1]
    gain_full[core] = gain_value
    gain_back = remote(
        gain_full.at[core], gain_full.at[core], gain_ss.at[chips], gain_rs.at[chips], partner
    )
    gain_back.start()

    for direction, h in ring_order:
        pass_on(direction, h, 1).wait_recv()
    normed_grad = jnp.concatenate(
        [
            held(0, h) + ring_recv[0, h, 0].astype(f32) + ring_recv[1, h, 0].astype(f32)
            for h in (0, 1)
        ],
        axis=1,
    )
    first = pl.ds(0, rows)
    norm_scale = scale[first, :]
    unit_rows = res[first, :].astype(f32) * norm_scale
    unit_grad = normed_grad * gain_ref[...]
    inner_mean = jnp.mean(unit_grad * unit_rows, axis=1, keepdims=True)
    grad_res_ref[...] = (
        ups[first, :].astype(f32) + norm_scale * (unit_grad - unit_rows * inner_mean)
    ).astype(bf16)

    gain_back.wait_recv()
    gain_out_ref[...] = gain_full[...]

    for direction, a in streams:
        for distance in range(reach(direction, a)):
            hop(direction, a, distance).wait_send()
            pass_on(direction, a, distance + 1).wait_send()
    for a in (0, 1):
        for k in range(chips):
            share(a, k).wait_send()
        swap(a).wait_send()
    gain_swap.wait_send()
    gain_back.wait_send()
    for copy in spread:
        copy.wait_send()
    for copy in outs:
        copy.wait()


def weight_kernel(
    normed_t, ups, hidden_t, gate_grad, up_grad, residual_in, gain_in,
    residual_out, gate_out, up_out, down_out, gain_out,
):
    rows_in = normed_t[...]
    gate_out[...] = jnp.dot(rows_in, gate_grad[...], preferred_element_type=f32).astype(bf16)
    up_out[...] = jnp.dot(rows_in, up_grad[...], preferred_element_type=f32).astype(bf16)
    down_out[...] = jnp.dot(hidden_t[...], ups[...], preferred_element_type=f32).astype(bf16)

    @pl.when(pl.program_id(0) == 0)
    def _():
        residual_out[...] = residual_in[...]
        gain_out[...] = gain_in[...]


def per_device(chips, residual, upstream, gate_weight, up_weight, down_weight, gain):
    rows, width = residual.shape
    units = gate_weight.shape[1]
    tokens = rows * 2 * chips
    half_ring = chips // 2
    shape = jax.ShapeDtypeStruct
    anywhere = pl.BlockSpec(memory_space=pl.ANY)
    in_vmem = pl.BlockSpec(memory_space=pltpu.VMEM)
    dma = pltpu.SemaphoreType.DMA
    grad_residual, grad_gain, normed, upstream_all, hidden, gate_grad, up_grad = pl.pallas_call(
        functools.partial(exchange_kernel, chips),
        out_shape=(
            shape((rows, width), bf16),
            shape((2, 1, width // 2), f32),
            shape((width, tokens), bf16),
            shape((tokens, width), bf16),
            shape((units, tokens), bf16),
            shape((tokens, units), bf16),
            shape((tokens, units), bf16),
        ),
        in_specs=[anywhere] * 5 + [in_vmem],
        out_specs=(in_vmem, in_vmem) + (anywhere,) * 5,
        scratch_shapes=[
            pltpu.VMEM((width, units), bf16),
            pltpu.VMEM((width, units), bf16),
            pltpu.VMEM((units, width), bf16),
            pltpu.VMEM((tokens, width), bf16),
            pltpu.VMEM((tokens, width), bf16),
            pltpu.VMEM((tokens, width), bf16),
            pltpu.VMEM((width, tokens), bf16),
            pltpu.VMEM((tokens, 1), f32),
            pltpu.VMEM((units, tokens), bf16),
            pltpu.VMEM((tokens, units), bf16),
            pltpu.VMEM((tokens, units), bf16),
            pltpu.VMEM((tokens, width), f32),
            pltpu.VMEM((tokens // 2, width), bf16),
            pltpu.VMEM((tokens // 2, width), bf16),
            pltpu.VMEM((2, 2, half_ring, rows, width // 2), bf16),
            pltpu.VMEM((2, 2, half_ring, rows, width // 2), bf16),
            pltpu.VMEM((2, 1, width // 2), f32),
            pltpu.VMEM((1, width // 2), f32),
            pltpu.VMEM((1, width // 2), f32),
            pltpu.VMEM((chips - 1, 1, width // 2), f32),
            pltpu.VMEM((2, 1, width // 2), f32),
            dma((3,)),
            dma((5,)),
            dma((2,)),
            dma((2, 2, half_ring)),
            dma((2, 2, half_ring)),
            dma((2, chips)),
            dma((2, chips)),
            dma((2,)),
            dma((2,)),
            dma((2, 2, half_ring)),
            dma((2, 2, half_ring)),
            dma((chips + 1,)),
            dma((chips + 1,)),
        ],
        compiler_params=pltpu.CompilerParams(
            collective_id=0, has_side_effects=True, vmem_limit_bytes=60 * 1024 * 1024
        ),
    )(residual, upstream, gate_weight, up_weight, down_weight, gain.reshape(1, width))
    steps = 6
    tile = width // steps
    whole = lambda *dims: pl.BlockSpec(dims, lambda i: (0,) * len(dims))
    down_rows = pl.BlockSpec((tile, units), lambda i: (i, 0))
    grad_residual, grad_gate, grad_up, grad_down, grad_gain = pl.pallas_call(
        weight_kernel,
        grid=(steps,),
        out_shape=(
            shape((rows, width), bf16),
            shape((width, units), bf16),
            shape((width, units), bf16),
            shape((units, width), bf16),
            shape((2, 1, width // 2), f32),
        ),
        in_specs=[
            pl.BlockSpec((tile, tokens), lambda i: (i, 0)),
            pl.BlockSpec((tokens, tile), lambda i: (0, i)),
            whole(units, tokens),
            whole(tokens, units),
            whole(tokens, units),
            whole(rows, width),
            whole(2, 1, width // 2),
        ],
        out_specs=(
            whole(rows, width),
            down_rows,
            down_rows,
            pl.BlockSpec((units, tile), lambda i: (0, i)),
            whole(2, 1, width // 2),
        ),
        compiler_params=pltpu.CompilerParams(vmem_limit_bytes=40 * 1024 * 1024),
        cost_estimate=pl.CostEstimate(
            flops=6 * tokens * width * units, bytes_accessed=8 * width * units, transcendentals=0
        ),
    )(normed, upstream_all, hidden, gate_grad, up_grad, grad_residual, grad_gain)
    return (grad_residual, grad_gate, grad_up, grad_down, grad_gain.reshape(width))


def solution(mesh):
    placed = (
        P(("member", "dp"), None),
        P(("member", "dp"), None),
        P("member", "dp"),
        P("member", "dp"),
        P(("member", "dp"), None),
        P("member"),
    )
    return jax.shard_map(
        functools.partial(per_device, mesh.shape["dp"] // 2),
        mesh=mesh,
        in_specs=placed,
        out_specs=(
            P(("member", "dp"), None),
            P("member", "dp"),
            P("member", "dp"),
            P(("member", "dp"), None),
            P("member"),
        ),
        check_vma=False,
    )
```

```python
import functools

import jax
import jax.numpy as jnp
from jax import lax
from jax.experimental import pallas as pl
from jax.experimental.pallas import tpu as pltpu
from jax.sharding import PartitionSpec as P

norm_floor = 0.5
gelu_coeff = 0.7978845608
cubic_term = 0.044715
MESH = pl.DeviceIdType.MESH
bf16, f32 = jnp.bfloat16, jnp.float32


def gelu_parts(gate_out):
    inner = jnp.tanh(gelu_coeff * (gate_out + cubic_term * gate_out * gate_out * gate_out))
    activated = 0.5 * gate_out * (1.0 + inner)
    gelu_slope = 0.5 * (1.0 + inner) + 0.5 * gate_out * (1.0 - inner * inner) * gelu_coeff * (
        1.0 + 3.0 * cubic_term * gate_out * gate_out
    )
    return (activated, gelu_slope)


def contract_last(left, right):
    return lax.dot_general(left, right, (((1,), (1,)), ((), ())), preferred_element_type=f32)


def contract_first(left, right):
    return lax.dot_general(left, right, (((0,), (0,)), ((), ())), preferred_element_type=f32)


def slot(side, distance, half_ring):
    if distance == half_ring:
        return 2 * half_ring - 1
    return 0 if distance == 0 else 2 * distance - 1 + side


def exchange_kernel(
    chips,
    res_hbm, ups_hbm, gate_hbm, up_hbm, down_hbm, gain_ref,
    grad_res_ref, gain_out_ref, normed_hbm, upstream_hbm, hidden_hbm, gate_grad_hbm, up_grad_hbm,
    gate_w, up_w, down_w, res, ups, normed, normed_t, scale, hidden, gate_grad, up_grad,
    part, peer_send, peer_recv, ring_send, ring_recv,
    gain_part, gain_peer, gain_sum, gain_all, gain_full,
    local_sem, out_sem, own_sem, ring_ss, ring_rs, peer_ss, peer_rs,
    swap_ss, swap_rs, sum_ss, sum_rs, gain_ss, gain_rs,
):
    half_ring = chips // 2
    rows = res_hbm.shape[0]
    width = res.shape[1]
    half_width = width // 2
    tokens = res.shape[0]
    me = lax.axis_index("dp")
    chip, core = me // 2, me % 2
    position = chip // 2 + (chip % 2) * (chips - 1 - 2 * (chip // 2))

    def device_at(place, which):
        place = (place + chips) % chips
        far = place // half_ring
        return 2 * ((1 - far) * (2 * place) + far * (2 * (chips - 1 - place) + 1)) + which

    partner = {"dp": 2 * chip + (1 - core)}
    onward = ({"dp": device_at(position + 1, core)}, {"dp": device_at(position - 1, core)})

    def block(ref, k, who):
        return ref.at[pl.ds((2 * k + who) * rows, rows)]

    sources, arrays = (res_hbm, ups_hbm), (res, ups)
    own = [pltpu.make_async_copy(sources[a], block(arrays[a], 0, 0), own_sem.at[a]) for a in (0, 1)]
    for copy in own:
        copy.start()
    weights = [
        pltpu.make_async_copy(src, dst, local_sem.at[i])
        for i, (src, dst) in enumerate(((gate_hbm, gate_w), (up_hbm, up_w), (down_hbm, down_w)))
    ]
    for copy in weights:
        copy.start()

    barrier = pltpu.get_barrier_semaphore()
    pl.semaphore_signal(barrier, inc=1, device_id=partner, device_id_type=MESH)
    for step in range(1, chips):
        pl.semaphore_signal(
            barrier, inc=1, device_id={"dp": device_at(position + step, core)}, device_id_type=MESH
        )
    pl.semaphore_wait(barrier, chips)
    for copy in own:
        copy.wait()

    def remote(src, dst, send, recv, target):
        return pltpu.make_async_remote_copy(
            src_ref=src, dst_ref=dst, send_sem=send, recv_sem=recv,
            device_id=target, device_id_type=MESH,
        )

    def reach(direction, a):
        return half_ring if direction == a else half_ring - 1

    def hop(direction, a, distance):
        return remote(
            block(arrays[a], slot(direction, distance, half_ring), 0),
            block(arrays[a], slot(direction, distance + 1, half_ring), 0),
            ring_ss.at[direction, a, distance],
            ring_rs.at[direction, a, distance],
            onward[direction],
        )

    def share(a, k):
        return remote(
            block(arrays[a], k, 0), block(arrays[a], k, 1),
            peer_ss.at[a, k], peer_rs.at[a, k], partner,
        )

    streams = [(0, 0), (1, 0), (0, 1), (1, 1)]
    for direction, a in streams:
        hop(direction, a, 0).start()
    for a in (0, 1):
        share(a, 0).start()

    def arrive(distance):
        for direction, a in streams:
            if distance > reach(direction, a):
                continue
            hop(direction, a, distance - 1).wait_recv()
            if distance < reach(direction, a):
                hop(direction, a, distance).start()
            share(a, slot(direction, distance, half_ring)).start()

    batch = chips // 2
    span = batch * 2 * rows

    def normalise(b):
        for k in range(b * batch, (b + 1) * batch):
            share(0, k).wait_recv()
            at = pl.ds(2 * k * rows, 2 * rows)
            wide = res[at, :].astype(f32)
            own_scale = lax.rsqrt(jnp.mean(wide * wide, axis=1, keepdims=True) + norm_floor)
            scale[at, :] = own_scale
            normed[at, :] = (wide * own_scale * gain_ref[...]).astype(bf16)

    def forward(b):
        at = pl.ds(b * span, span)
        rows_in = normed[at, :]
        gate_out = jnp.dot(rows_in, gate_w[...], preferred_element_type=f32)
        up_out = jnp.dot(rows_in, up_w[...], preferred_element_type=f32)
        for k in range(b * batch, (b + 1) * batch):
            share(1, k).wait_recv()
        hidden_grad = contract_last(ups[at, :], down_w[...])
        activated, gelu_slope = gelu_parts(gate_out)
        hidden[:, at] = (activated * up_out).T.astype(bf16)
        gate_grad[at, :] = (hidden_grad * up_out * gelu_slope).astype(bf16)
        up_grad[at, :] = (hidden_grad * activated).astype(bf16)

    def backward(b):
        at = pl.ds(b * span, span)
        part[at, :] = contract_last(gate_grad[at, :], gate_w[...]) + contract_last(
            up_grad[at, :], up_w[...]
        )
        for k in range(b * batch, (b + 1) * batch):
            peer_send[pl.ds(k * rows, rows), :] = part[pl.ds((2 * k + 1) * rows, rows), :].astype(bf16)
        swap(b).start()

    def swap(b):
        at = pl.ds(b * batch * rows, batch * rows)
        return remote(peer_send.at[at], peer_recv.at[at], swap_ss.at[b], swap_rs.at[b], partner)

    def turn(b):
        at = pl.ds(b * span, span)
        normed_t[:, at] = normed[at, :].T

    def gain_term(b):
        total = jnp.zeros((1, width), f32)
        for k in range(b * batch, (b + 1) * batch):
            at = pl.ds(2 * k * rows, 2 * rows)
            unit_rows = res[at, :].astype(f32) * scale[at, :]
            total = total + jnp.sum(part[at, :] * unit_rows, axis=0, keepdims=True)
        return total

    early = (half_ring + 1) // 2
    for distance in range(1, early + 1):
        arrive(distance)
    for copy in weights:
        copy.wait()
    normalise(0)
    forward(0)
    for distance in range(early + 1, half_ring):
        arrive(distance)
    backward(0)
    gain_total = gain_term(0)
    turn(0)
    arrive(half_ring)
    normalise(1)
    forward(1)
    backward(1)

    def pass_on(direction, h, distance):
        return remote(
            ring_send.at[direction, h, distance - 1],
            ring_recv.at[direction, h, distance - 1],
            sum_ss.at[direction, h, distance - 1],
            sum_rs.at[direction, h, distance - 1],
            onward[direction],
        )

    def columns(h):
        return pl.ds(h * half_width, half_width)

    def held(k, h):
        return part[pl.ds(2 * k * rows, rows), columns(h)] + peer_recv[
            pl.ds(k * rows, rows), columns(h)
        ].astype(f32)

    ring_order = [(0, 0), (1, 1), (1, 0), (0, 1)]

    def sum_step(distance):
        for direction, h in ring_order:
            if distance > reach(direction, h):
                continue
            value = held(slot(1 - direction, distance, half_ring), h)
            if distance < reach(direction, h):
                pass_on(direction, h, distance + 1).wait_recv()
                value = value + ring_recv[direction, h, distance].astype(f32)
            ring_send[direction, h, distance - 1] = value.astype(bf16)
            pass_on(direction, h, distance).start()

    swap(1).wait_recv()
    sum_step(half_ring)

    gain_total = gain_total + gain_term(1)
    gain_part[0] = gain_total[:, :half_width]
    gain_part[1] = gain_total[:, half_width:]
    gain_swap = remote(gain_part.at[1 - core], gain_peer, gain_ss.at[0], gain_rs.at[0], partner)
    gain_swap.start()
    swap(0).wait_recv()

    sum_step(half_ring - 1)
    turn(1)
    outs = [
        pltpu.make_async_copy(src, dst, out_sem.at[i])
        for i, (src, dst) in enumerate(
            (
                (normed_t, normed_hbm), (ups, upstream_hbm), (hidden, hidden_hbm),
                (gate_grad, gate_grad_hbm), (up_grad, up_grad_hbm),
            )
        )
    ]
    for copy in outs:
        copy.start()

    gain_swap.wait_recv()
    gain_sum[...] = gain_part[core] + gain_peer[...]
    spread = [
        remote(
            gain_sum, gain_all.at[step - 1], gain_ss.at[step], gain_rs.at[step],
            {"dp": device_at(position + step, core)},
        )
        for step in range(1, chips)
    ]
    for copy in spread:
        copy.start()
    for distance in range(half_ring - 2, 0, -1):
        sum_step(distance)

    gain_value = gain_sum[...]
    for step in range(1, chips):
        spread[step - 1].wait_recv()
        gain_value = gain_value + gain_all[step - 1]
    gain_full[core] = gain_value
    gain_back = remote(
        gain_full.at[core], gain_full.at[core], gain_ss.at[chips], gain_rs.at[chips], partner
    )
    gain_back.start()

    for direction, h in ring_order:
        pass_on(direction, h, 1).wait_recv()
    normed_grad = jnp.concatenate(
        [
            held(0, h) + ring_recv[0, h, 0].astype(f32) + ring_recv[1, h, 0].astype(f32)
            for h in (0, 1)
        ],
        axis=1,
    )
    first = pl.ds(0, rows)
    norm_scale = scale[first, :]
    unit_rows = res[first, :].astype(f32) * norm_scale
    unit_grad = normed_grad * gain_ref[...]
    inner_mean = jnp.mean(unit_grad * unit_rows, axis=1, keepdims=True)
    grad_res_ref[...] = (
        ups[first, :].astype(f32) + norm_scale * (unit_grad - unit_rows * inner_mean)
    ).astype(bf16)

    gain_back.wait_recv()
    gain_out_ref[...] = gain_full[...]

    for direction, a in streams:
        for distance in range(reach(direction, a)):
            hop(direction, a, distance).wait_send()
            pass_on(direction, a, distance + 1).wait_send()
    for a in (0, 1):
        for k in range(chips):
            share(a, k).wait_send()
        swap(a).wait_send()
    gain_swap.wait_send()
    gain_back.wait_send()
    for copy in spread:
        copy.wait_send()
    for copy in outs:
        copy.wait()


def weight_kernel(
    normed_t, ups, hidden_t, gate_grad, up_grad, residual_in, gain_in,
    residual_out, gate_out, up_out, down_out, gain_out,
):
    rows_in = normed_t[...]
    gate_out[...] = jnp.dot(rows_in, gate_grad[...], preferred_element_type=f32).astype(bf16)
    up_out[...] = jnp.dot(rows_in, up_grad[...], preferred_element_type=f32).astype(bf16)
    down_out[...] = jnp.dot(hidden_t[...], ups[...], preferred_element_type=f32).astype(bf16)

    @pl.when(pl.program_id(0) == 0)
    def _():
        residual_out[...] = residual_in[...]
        gain_out[...] = gain_in[...]


def per_device(chips, residual, upstream, gate_weight, up_weight, down_weight, gain):
    rows, width = residual.shape
    units = gate_weight.shape[1]
    tokens = rows * 2 * chips
    half_ring = chips // 2
    shape = jax.ShapeDtypeStruct
    anywhere = pl.BlockSpec(memory_space=pl.ANY)
    in_vmem = pl.BlockSpec(memory_space=pltpu.VMEM)
    dma = pltpu.SemaphoreType.DMA
    grad_residual, grad_gain, normed, upstream_all, hidden, gate_grad, up_grad = pl.pallas_call(
        functools.partial(exchange_kernel, chips),
        out_shape=(
            shape((rows, width), bf16),
            shape((2, 1, width // 2), f32),
            shape((width, tokens), bf16),
            shape((tokens, width), bf16),
            shape((units, tokens), bf16),
            shape((tokens, units), bf16),
            shape((tokens, units), bf16),
        ),
        in_specs=[anywhere] * 5 + [in_vmem],
        out_specs=(in_vmem, in_vmem) + (anywhere,) * 5,
        scratch_shapes=[
            pltpu.VMEM((width, units), bf16),
            pltpu.VMEM((width, units), bf16),
            pltpu.VMEM((units, width), bf16),
            pltpu.VMEM((tokens, width), bf16),
            pltpu.VMEM((tokens, width), bf16),
            pltpu.VMEM((tokens, width), bf16),
            pltpu.VMEM((width, tokens), bf16),
            pltpu.VMEM((tokens, 1), f32),
            pltpu.VMEM((units, tokens), bf16),
            pltpu.VMEM((tokens, units), bf16),
            pltpu.VMEM((tokens, units), bf16),
            pltpu.VMEM((tokens, width), f32),
            pltpu.VMEM((tokens // 2, width), bf16),
            pltpu.VMEM((tokens // 2, width), bf16),
            pltpu.VMEM((2, 2, half_ring, rows, width // 2), bf16),
            pltpu.VMEM((2, 2, half_ring, rows, width // 2), bf16),
            pltpu.VMEM((2, 1, width // 2), f32),
            pltpu.VMEM((1, width // 2), f32),
            pltpu.VMEM((1, width // 2), f32),
            pltpu.VMEM((chips - 1, 1, width // 2), f32),
            pltpu.VMEM((2, 1, width // 2), f32),
            dma((3,)),
            dma((5,)),
            dma((2,)),
            dma((2, 2, half_ring)),
            dma((2, 2, half_ring)),
            dma((2, chips)),
            dma((2, chips)),
            dma((2,)),
            dma((2,)),
            dma((2, 2, half_ring)),
            dma((2, 2, half_ring)),
            dma((chips + 1,)),
            dma((chips + 1,)),
        ],
        compiler_params=pltpu.CompilerParams(
            collective_id=0, has_side_effects=True, vmem_limit_bytes=60 * 1024 * 1024
        ),
    )(residual, upstream, gate_weight, up_weight, down_weight, gain.reshape(1, width))
    steps = 6
    tile = width // steps
    whole = lambda *dims: pl.BlockSpec(dims, lambda i: (0,) * len(dims))
    down_rows = pl.BlockSpec((tile, units), lambda i: (i, 0))
    grad_residual, grad_gate, grad_up, grad_down, grad_gain = pl.pallas_call(
        weight_kernel,
        grid=(steps,),
        out_shape=(
            shape((rows, width), bf16),
            shape((width, units), bf16),
            shape((width, units), bf16),
            shape((units, width), bf16),
            shape((2, 1, width // 2), f32),
        ),
        in_specs=[
            pl.BlockSpec((tile, tokens), lambda i: (i, 0)),
            pl.BlockSpec((tokens, tile), lambda i: (0, i)),
            whole(units, tokens),
            whole(tokens, units),
            whole(tokens, units),
            whole(rows, width),
            whole(2, 1, width // 2),
        ],
        out_specs=(
            whole(rows, width),
            down_rows,
            down_rows,
            pl.BlockSpec((units, tile), lambda i: (0, i)),
            whole(2, 1, width // 2),
        ),
        compiler_params=pltpu.CompilerParams(vmem_limit_bytes=62 * 1024 * 1024),
        cost_estimate=pl.CostEstimate(
            flops=6 * tokens * width * units, bytes_accessed=8 * width * units, transcendentals=0
        ),
    )(normed, upstream_all, hidden, gate_grad, up_grad, grad_residual, grad_gain)
    return (grad_residual, grad_gate, grad_up, grad_down, grad_gain.reshape(width))


def solution(mesh):
    placed = (
        P(("member", "dp"), None),
        P(("member", "dp"), None),
        P("member", "dp"),
        P("member", "dp"),
        P(("member", "dp"), None),
        P("member"),
    )
    return jax.shard_map(
        functools.partial(per_device, mesh.shape["dp"] // 2),
        mesh=mesh,
        in_specs=placed,
        out_specs=(
            P(("member", "dp"), None),
            P("member", "dp"),
            P("member", "dp"),
            P(("member", "dp"), None),
            P("member"),
        ),
        check_vma=False,
    )
```
